32 devices in a mesh: gx: 4 (over y, x), gy: 2 (over core), gz: 4 (over z).
Axes of the slice: x: 2, y: 2, z: 4, core: 2. Of those that a mesh axis runs over, the one named last changes fastest.
Arguments:
- states: float32 [41, 16, 32, 1024], P(None, 'gz', 'gy', 'gx'), may hold values from 0 to 1
- prior_states: float32 [41, 16, 32, 1024], P(None, 'gz', 'gy', 'gx'), may hold values from 0 to 1
- cell_layers: int32 [16, 32, 1024], P('gz', 'gy', 'gx'), may hold values from 0 to 2
- fiber_classes: int32 [16, 32, 1024], P('gz', 'gy', 'gx'), may hold values from 0 to 15
- writer_stripe: int32 [8], replicated, may hold values from 0 to 7, each once
- gate_half: float32 [3, 40], replicated, may hold values from -1 to 1.5
- gate_slope: float32 [3, 40], replicated, may hold values from 1 to 8
- gate_tau: float32 [3, 40], replicated, may hold values from 1 to 40
- gate_conduct: float32 [3, 40], replicated, may hold values from 0.002 to 0.025
- gate_reversal: float32 [3, 40], replicated, may hold values from -1.5 to 1.5
- fiber_conduct: float32 [16, 3], replicated, may hold values from 0.02 to 0.15
Outputs:
- new_states: float32 [41, 16, 32, 1024], P(None, 'gz', 'gy', 'gx')
- stripes: float32 [41, 64, 8, 1024], P(None, ('gy', 'gz'), None, 'gx')
The draws below stay inside these ranges and needn't reach their ends.
Inputs may be any that keep to these rules, and one draw needn't show every extreme that they name: `writer_stripe`: every one of the 8 stripes has exactly one writer.
All inputs are finite; a program needn't handle non-finite values.
Results may differ from the reference program's by a relative error of at most 0.000062.
Values sent between devices are 32-bit elements; how exact they have to be, the bound alone decides.
A program may use at most 64 MiB of HBM per device.

```python
import math
import jax
import jax.numpy as jnp
from jax import lax

STATES = 41
GATES = 40
LAYERS = 3
FIBERS = 16
STEPS = 4
CT = 4
CW = 16
NT = 16
NW = 32
ND = 1024
WRITERS = 8
ROWS = 8
STRIPES = 64
N_GY = 2
N_GZ = 4


def with_ends(values, key, least, high):
    spot = [jax.random.randint(jax.random.fold_in(key, axis), (), 0, length) for axis, length in enumerate(values.shape)]
    main_axis = values.shape.index(max(values.shape))
    neighbour = spot[:main_axis] + [(spot[main_axis] + 1) % values.shape[main_axis]] + spot[main_axis + 1:]
    return values.at[tuple(spot)].set(least).at[tuple(neighbour)].set(high)


def block_levels(stream_key, dims, cuts, smallest, high):
    def one(dim, shards_of):
        heights = jax.random.uniform(jax.random.fold_in(jax.random.fold_in(stream_key, 6), dim), (shards_of,), jnp.float32, smallest / len(cuts), high / len(cuts))
        return jnp.repeat(jnp.exp(heights), dims[dim] // shards_of).reshape((-1,) + (1,) * (len(dims) - dim - 1))

    gain = one(*cuts[0])
    for cut in cuts[1:]:
        gain = gain * one(*cut)
    return gain


def setup_inputs(seed: int = 0) -> dict:
    keys = jax.random.split(jax.random.key(seed), 12)
    states = jnp.clip(1.0 * jax.random.uniform(keys[0], (STATES, NT, NW, ND), jnp.float32) ** block_levels(keys[0], (STATES, NT, NW, ND), ((1, 4), (2, 2), (3, 4)), -0.2, 0.2), 0.0, 1.0)
    prior_states = jnp.clip(1.0 * jax.random.uniform(keys[1], (STATES, NT, NW, ND), jnp.float32) ** block_levels(keys[1], (STATES, NT, NW, ND), ((1, 4), (2, 2), (3, 4)), -0.2, 0.2), 0.0, 1.0)
    cell_layers = with_ends(jax.random.randint(keys[2], (NT, NW, ND), 0, LAYERS), jax.random.fold_in(keys[2], 1), 0, LAYERS - 1).astype(jnp.int32)
    fiber_classes = with_ends(jax.random.randint(keys[3], (NT, NW, ND), 0, FIBERS), jax.random.fold_in(keys[3], 1), 0, FIBERS - 1).astype(jnp.int32)
    writer_stripe = jax.random.permutation(keys[4], WRITERS).astype(jnp.int32)
    gate_half = jnp.clip(jax.random.uniform(keys[5], (LAYERS, GATES), jnp.float32, -1.0, 1.5), -1.0, 1.5)
    gate_slope = jnp.clip(jnp.exp(jax.random.uniform(keys[6], (LAYERS, GATES), jnp.float32, math.log(1.0), math.log(8.0))), 1.0, 8.0)
    gate_tau = jnp.clip(jnp.exp(jax.random.uniform(keys[7], (LAYERS, GATES), jnp.float32, math.log(1.0), math.log(40.0))), 1.0, 40.0)
    gate_conduct = jnp.clip(jnp.exp(jax.random.uniform(keys[8], (LAYERS, GATES), jnp.float32, math.log(0.002), math.log(0.025))), 0.002, 0.025)
    gate_reversal = jnp.clip(jax.random.uniform(keys[9], (LAYERS, GATES), jnp.float32, -1.5, 1.5), -1.5, 1.5)
    fiber_conduct = jnp.clip(jax.random.uniform(keys[10], (FIBERS, 3), jnp.float32, 0.02, 0.15), 0.02, 0.15)
    return {"states": states, "prior_states": prior_states, "cell_layers": cell_layers, "fiber_classes": fiber_classes, "writer_stripe": writer_stripe, "gate_half": gate_half, "gate_slope": gate_slope, "gate_tau": gate_tau, "gate_conduct": gate_conduct, "gate_reversal": gate_reversal, "fiber_conduct": fiber_conduct}


def pick_layer(cell_layers, column):
    picked = jnp.zeros(cell_layers.shape, jnp.float32) + column[LAYERS - 1]
    for which_layer in range(LAYERS - 2, -1, -1):
        picked = jnp.where(cell_layers == which_layer, column[which_layer], picked)
    return picked


def ionic_update(voltage, gate_states, cell_layers, gate_half, gate_slope, gate_tau, gate_conduct, gate_reversal):
    def one_gate(current, inputs):
        half_row, slope_row, tau_row, cond_row, rev_row, gate_now = inputs
        steady = jax.nn.sigmoid((voltage - pick_layer(cell_layers, half_row)) * pick_layer(cell_layers, slope_row))
        decay_rate = jnp.exp(-1.0 / (pick_layer(cell_layers, tau_row) * (1.0 + steady)))
        gate_next = steady + (gate_now - steady) * decay_rate
        current = current + pick_layer(cell_layers, cond_row) * gate_next * (voltage - pick_layer(cell_layers, rev_row))
        return current, gate_next

    inputs = (gate_half.T, gate_slope.T, gate_tau.T, gate_conduct.T, gate_reversal.T, gate_states)
    current, gate_next = lax.scan(one_gate, jnp.zeros_like(voltage), inputs)
    return voltage - current, gate_next


def diffuse(excited, sigma_cells):
    padded = jnp.pad(excited, 1, mode="edge")
    centre = excited
    across = (padded[2:, 1:-1, 1:-1] - centre) + (padded[:-2, 1:-1, 1:-1] - centre)
    widthwise = (padded[1:-1, 2:, 1:-1] - centre) + (padded[1:-1, :-2, 1:-1] - centre)
    depthwise = (padded[1:-1, 1:-1, 2:] - centre) + (padded[1:-1, 1:-1, :-2] - centre)
    return excited + sigma_cells[..., 0] * across + sigma_cells[..., 1] * widthwise + sigma_cells[..., 2] * depthwise


def reference(states, prior_states, cell_layers, fiber_classes, writer_stripe, gate_half, gate_slope, gate_tau, gate_conduct, gate_reversal, fiber_conduct):
    sigma_cells = fiber_conduct[fiber_classes]
    voltage = states[0]
    gate_states = states[1:]
    for step_index in range(STEPS):
        excited, gate_states = ionic_update(voltage, gate_states, cell_layers, gate_half, gate_slope, gate_tau, gate_conduct, gate_reversal)
        voltage = diffuse(excited, sigma_cells)
    new_states = jnp.concatenate([voltage[None], gate_states], axis=0)
    blocks = prior_states.reshape(STATES, N_GZ, CT, N_GY, CW, ND)
    blocks = jnp.transpose(blocks, (0, 3, 1, 2, 4, 5)).reshape(STATES, WRITERS, WRITERS, ROWS, ND)
    chosen = jnp.take(blocks, writer_stripe, axis=2)
    stripes = jnp.transpose(chosen, (0, 2, 1, 3, 4)).reshape(STATES, STRIPES, ROWS, ND)
    return new_states, stripes
```

```python
import functools

import jax
import jax.numpy as jnp
from jax import lax
from jax.experimental import pallas as pl
from jax.experimental.pallas import tpu as pltpu
from jax.sharding import PartitionSpec as P

STEPS = 4
MESH = pl.DeviceIdType.MESH
SUB = 8
LANES = 128
LO_T, HI_T, LO_W, HI_W, LO_D, HI_D = range(6)


def kernel(
    sizes,
    states_hbm,
    prior_hbm,
    layers_ref,
    fibers_ref,
    stripe_ref,
    half_ref,
    slope_ref,
    tau_ref,
    cond_ref,
    rev_ref,
    conduct_ref,
    new_hbm,
    arrived_hbm,
    cells,
    prior,
    outgoing,
    excited,
    face_lo_t,
    face_hi_t,
    face_lo_w,
    face_hi_w,
    face_lo_d,
    face_hi_d,
    sigma,
    load_sem,
    store_sem,
    send_sem,
    recv_sem,
    face_send,
    face_recv,
):
    n_gx, n_gy, n_gz = sizes
    writers = n_gy * n_gz
    states_count, cells_t, cells_w, cells_d = cells.shape
    rows = outgoing.shape[2]
    layer_count, gates = half_ref.shape
    gx, gy, gz = lax.axis_index("gx"), lax.axis_index("gy"), lax.axis_index("gz")
    me = gy * n_gz + gz

    load_prior = pltpu.make_async_copy(prior_hbm, prior, load_sem.at[0])
    load_cells = pltpu.make_async_copy(states_hbm, cells, load_sem.at[1])
    load_prior.start()
    load_cells.start()

    barrier = pltpu.get_barrier_semaphore()
    peers = 0
    for shift_y in range(n_gy):
        for shift_z in range(n_gz):
            if shift_y or shift_z:
                target = (gx, lax.rem(gy + shift_y, n_gy), lax.rem(gz + shift_z, n_gz))
                pl.semaphore_signal(barrier, inc=1, device_id=target, device_id_type=MESH)
                peers += 1
    if n_gx > 1:
        for shift in (1, n_gx - 1):
            target = (lax.rem(gx + shift, n_gx), gy, gz)
            pl.semaphore_signal(barrier, inc=1, device_id=target, device_id_type=MESH)
            peers += 1

    load_prior.wait()
    for writer in range(writers):
        outgoing[writer] = prior[:, stripe_ref[writer]]
    if peers:
        pl.semaphore_wait(barrier, peers)

    def piece(target_gy, target_gz):
        target = target_gy * n_gz + target_gz
        return pltpu.make_async_remote_copy(
            src_ref=outgoing.at[target],
            dst_ref=arrived_hbm.at[me],
            send_sem=send_sem.at[target],
            recv_sem=recv_sem.at[me],
            device_id=(gx, target_gy, target_gz),
            device_id_type=MESH,
        )

    batches = [(distance, shift_y) for distance in range(1, n_gz) for shift_y in range(n_gy)]

    def start_batch(batch):
        distance, shift_y = batch
        target_gy = lax.rem(gy + shift_y, n_gy)

        @pl.when(gz + distance < n_gz)
        def _():
            piece(target_gy, gz + distance).start()

        @pl.when(gz >= distance)
        def _():
            piece(target_gy, gz - distance).start()

    per_step = [batches[i : i + 1] for i in range(STEPS)] + [batches[STEPS:]]
    for batch in per_step[0]:
        start_batch(batch)
    for shift_y in range(1, n_gy):
        piece(lax.rem(gy + shift_y, n_gy), gz).start()
    own = pltpu.make_async_copy(outgoing.at[me], arrived_hbm.at[me], load_sem.at[2])
    own.start()

    at_lo = {LO_T: gz == 0, LO_W: gy == 0, LO_D: gx == 0}
    at_hi = {HI_T: gz == n_gz - 1, HI_W: gy == n_gy - 1, HI_D: gx == n_gx - 1}
    landing = {
        LO_T: face_lo_t, HI_T: face_hi_t, LO_W: face_lo_w,
        HI_W: face_hi_w, LO_D: face_lo_d, HI_D: face_hi_d,
    }
    missing = {**at_lo, **at_hi}
    no_target = {
        LO_T: at_hi[HI_T], HI_T: at_lo[LO_T], LO_W: at_hi[HI_W],
        HI_W: at_lo[LO_W], LO_D: at_hi[HI_D], HI_D: at_lo[LO_D],
    }
    for face, ref in landing.items():
        @pl.when(missing[face])
        def _(ref=ref):
            ref[...] = jnp.zeros_like(ref)

    def face_copy(step, face):
        sources = {
            LO_T: (excited.at[step, cells_t - 1], (gx, gy, gz + 1)),
            HI_T: (excited.at[step, 0], (gx, gy, gz - 1)),
            LO_W: (excited.at[step, :, pl.ds(cells_w - SUB, SUB), :], (gx, gy + 1, gz)),
            HI_W: (excited.at[step, :, pl.ds(0, SUB), :], (gx, gy - 1, gz)),
            LO_D: (excited.at[step, :, :, pl.ds(cells_d - LANES, LANES)], (gx + 1, gy, gz)),
            HI_D: (excited.at[step, :, :, pl.ds(0, LANES)], (gx - 1, gy, gz)),
        }
        source, target = sources[face]
        return pltpu.make_async_remote_copy(
            src_ref=source,
            dst_ref=landing[face].at[step],
            send_sem=face_send.at[step, face],
            recv_sem=face_recv.at[step, face],
            device_id=target,
            device_id_type=MESH,
        )

    classes = fibers_ref[...]
    picked = [jnp.full(classes.shape, conduct_ref[0, c], jnp.float32) for c in range(3)]
    for fiber in range(1, conduct_ref.shape[0]):
        hit = classes == fiber
        picked = [jnp.where(hit, conduct_ref[fiber, c], old) for c, old in enumerate(picked)]
    for c in range(3):
        sigma[c] = picked[c]

    load_cells.wait()
    slab = max(1, cells_t // 2)

    def ionic(step):
        for first in range(0, cells_t, slab):
            span = pl.ds(first, slab)
            voltage = cells[0, span]
            layer = layers_ref[span]
            hits = [layer == which for which in range(layer_count - 1)]

            def pick(table, gate):
                value = jnp.full(voltage.shape, table[layer_count - 1, gate], jnp.float32)
                for which in range(layer_count - 2, -1, -1):
                    value = jnp.where(hits[which], table[which, gate], value)
                return value

            def one_gate(gate, current):
                steady = 1.0 / (
                    1.0 + jnp.exp((pick(half_ref, gate) - voltage) * pick(slope_ref, gate))
                )
                decay = jnp.exp(-1.0 / (pick(tau_ref, gate) * (1.0 + steady)))
                value = steady + (cells[gate + 1, span] - steady) * decay
                cells[gate + 1, span] = value
                return current + pick(cond_ref, gate) * value * (voltage - pick(rev_ref, gate))

            current = lax.fori_loop(0, gates, one_gate, jnp.zeros_like(voltage))
            excited[step, span] = voltage - current

    flat = (cells_t * cells_w, cells_d)
    row = lax.broadcasted_iota(jnp.int32, flat, 0) % cells_w
    lane = lax.broadcasted_iota(jnp.int32, flat, 1)

    def factor(flag):
        return 1.0 - flag.astype(jnp.float32)

    def spread(rows_value):
        return jnp.broadcast_to(rows_value, (cells_t, cells_w, cells_d)).reshape(flat)

    def diffuse(step):
        centre3 = excited[step]
        centre = centre3.reshape(flat)
        below = jnp.concatenate([face_lo_t[step][None], centre3[:-1]], axis=0) - centre3
        above = jnp.concatenate([centre3[1:], face_hi_t[step][None]], axis=0) - centre3
        slab_index = lax.broadcasted_iota(jnp.int32, centre3.shape, 0)
        below = jnp.where(slab_index == 0, below * factor(missing[LO_T]), below)
        above = jnp.where(slab_index == cells_t - 1, above * factor(missing[HI_T]), above)
        across = (below + above).reshape(flat)

        low = spread(face_lo_w[step][:, SUB - 1 : SUB, :])
        high = spread(face_hi_w[step][:, 0:1, :])
        below = jnp.where(
            row == 0, (low - centre) * factor(missing[LO_W]), pltpu.roll(centre, 1, 0) - centre
        )
        above = jnp.where(
            row == cells_w - 1,
            (high - centre) * factor(missing[HI_W]),
            pltpu.roll(centre, flat[0] - 1, 0) - centre,
        )
        widthwise = below + above

        low = pltpu.roll(face_lo_d[step].reshape(flat[0], LANES), 1, 1)
        high = pltpu.roll(face_hi_d[step].reshape(flat[0], LANES), LANES - 1, 1)
        low = jnp.concatenate([low] * (cells_d // LANES), axis=1)
        high = jnp.concatenate([high] * (cells_d // LANES), axis=1)
        below = jnp.where(
            lane == 0, (low - centre) * factor(missing[LO_D]), pltpu.roll(centre, 1, 1) - centre
        )
        above = jnp.where(
            lane == cells_d - 1,
            (high - centre) * factor(missing[HI_D]),
            pltpu.roll(centre, cells_d - 1, 1) - centre,
        )
        depthwise = below + above
        voltage = (
            centre
            + sigma[0].reshape(flat) * across
            + sigma[1].reshape(flat) * widthwise
            + sigma[2].reshape(flat) * depthwise
        )
        cells[0] = voltage.reshape(centre3.shape)

    store_gates = pltpu.make_async_copy(
        cells.at[pl.ds(1, gates)], new_hbm.at[pl.ds(1, gates)], store_sem.at[0]
    )
    store_voltage = pltpu.make_async_copy(cells.at[0], new_hbm.at[0], store_sem.at[1])
    for step in range(STEPS):
        ionic(step)
        for face in range(6):
            @pl.when(jnp.logical_not(no_target[face]))
            def _(face=face):
                face_copy(step, face).start()
        for batch in per_step[step + 1]:
            start_batch(batch)
        if step == STEPS - 1:
            store_gates.start()
        for face in range(6):
            @pl.when(jnp.logical_not(missing[face]))
            def _(face=face):
                face_copy(step, face).wait_recv()
        diffuse(step)
    store_voltage.start()

    for step in range(STEPS):
        for face in range(6):
            @pl.when(jnp.logical_not(no_target[face]))
            def _(face=face, step=step):
                face_copy(step, face).wait_send()
    own.wait()
    for shift_y in range(n_gy):
        for shift_z in range(n_gz):
            if shift_y or shift_z:
                source_gy = lax.rem(gy + shift_y, n_gy)
                source_gz = lax.rem(gz + shift_z, n_gz)
                source = source_gy * n_gz + source_gz
                piece(source_gy, source_gz).wait_send()
                pltpu.make_async_remote_copy(
                    src_ref=outgoing.at[source],
                    dst_ref=arrived_hbm.at[source],
                    send_sem=send_sem.at[source],
                    recv_sem=recv_sem.at[source],
                    device_id=(gx, source_gy, source_gz),
                    device_id_type=MESH,
                ).wait_recv()
    store_gates.wait()
    store_voltage.wait()


def per_device(sizes, states, prior_states, cell_layers, fiber_classes, writer_stripe, *tables):
    n_gx, n_gy, n_gz = sizes
    writers = n_gy * n_gz
    count, cells_t, cells_w, cells_d = states.shape
    rows = cells_t * cells_w // writers
    f32 = jnp.float32
    hbm = pl.BlockSpec(memory_space=pl.ANY)
    vmem = pl.BlockSpec(memory_space=pltpu.VMEM)
    smem = pl.BlockSpec(memory_space=pltpu.SMEM)
    new_states, arrived = pl.pallas_call(
        functools.partial(kernel, sizes),
        out_shape=(
            jax.ShapeDtypeStruct(states.shape, f32),
            jax.ShapeDtypeStruct((writers, count, rows, cells_d), f32),
        ),
        in_specs=[hbm, hbm, vmem, vmem] + [smem] * 7,
        out_specs=(hbm, hbm),
        scratch_shapes=[
            pltpu.VMEM(states.shape, f32),
            pltpu.VMEM((count, writers, rows, cells_d), f32),
            pltpu.VMEM((writers, count, rows, cells_d), f32),
            pltpu.VMEM((STEPS, cells_t, cells_w, cells_d), f32),
            pltpu.VMEM((STEPS, cells_w, cells_d), f32),
            pltpu.VMEM((STEPS, cells_w, cells_d), f32),
            pltpu.VMEM((STEPS, cells_t, SUB, cells_d), f32),
            pltpu.VMEM((STEPS, cells_t, SUB, cells_d), f32),
            pltpu.VMEM((STEPS, cells_t, cells_w, LANES), f32),
            pltpu.VMEM((STEPS, cells_t, cells_w, LANES), f32),
            pltpu.VMEM((3, cells_t, cells_w, cells_d), f32),
            pltpu.SemaphoreType.DMA((3,)),
            pltpu.SemaphoreType.DMA((2,)),
            pltpu.SemaphoreType.DMA((writers,)),
            pltpu.SemaphoreType.DMA((writers,)),
            pltpu.SemaphoreType.DMA((STEPS, 6)),
            pltpu.SemaphoreType.DMA((STEPS, 6)),
        ],
        compiler_params=pltpu.CompilerParams(
            collective_id=0, has_side_effects=True, vmem_limit_bytes=48 * 1024 * 1024
        ),
        name="monodomain",
    )(
        states,
        prior_states.reshape(count, writers, rows, cells_d),
        cell_layers,
        fiber_classes,
        writer_stripe,
        *tables,
    )
    return new_states, jnp.swapaxes(arrived, 0, 1)


def solution(mesh):
    cells = P("gz", "gy", "gx")
    whole_states = P(None, "gz", "gy", "gx")
    sizes = (mesh.shape["gx"], mesh.shape["gy"], mesh.shape["gz"])
    return jax.shard_map(
        functools.partial(per_device, sizes),
        mesh=mesh,
        in_specs=(whole_states, whole_states, cells, cells) + (P(),) * 7,
        out_specs=(whole_states, P(None, ("gy", "gz"), None, "gx")),
        check_vma=False,
    )
```

```python
import functools

import jax
import jax.numpy as jnp
from jax import lax
from jax.experimental import pallas as pl
from jax.experimental.pallas import tpu as pltpu
from jax.sharding import PartitionSpec as P

STEPS = 4
MESH = pl.DeviceIdType.MESH
SUB = 8
LANES = 128
OUT_CUTS = 4
VMEM_BYTES = 67_043_328
FIRST_BATCHES = 1
LO_T, HI_T, LO_W, HI_W, LO_D, HI_D = range(6)


def kernel(
    sizes,
    states_hbm,
    prior_hbm,
    *rest,
):
    small_hbm, (cells, arrived), scratch = rest[:9], rest[9:11], rest[11:]
    small, (prior, outgoing, excited, face_lo_t, face_hi_t, face_lo_w, face_hi_w, face_lo_d, face_hi_d, sigma, load_sem, small_sem, send_sem, recv_sem, face_send, face_recv) = scratch[:9], scratch[9:]
    layers_ref, fibers_ref, stripe_ref, half_ref, slope_ref, tau_ref, cond_ref, rev_ref, conduct_ref = small
    n_gx, n_gy, n_gz = sizes
    writers = n_gy * n_gz
    states_count, cells_t, cells_w, cells_d = cells.shape
    rows = outgoing.shape[2]
    layer_count, gates = half_ref.shape
    gx, gy, gz = lax.axis_index("gx"), lax.axis_index("gy"), lax.axis_index("gz")
    me = gy * n_gz + gz

    load_prior = pltpu.make_async_copy(prior_hbm, prior, load_sem.at[0])
    load_small = [
        pltpu.make_async_copy(source, target, small_sem.at[i])
        for i, (source, target) in enumerate(zip(small_hbm, small))
    ]
    load_cells = pltpu.make_async_copy(states_hbm, cells, load_sem.at[1])
    load_small[2].start()
    load_prior.start()
    for i, load in enumerate(load_small):
        if i != 2:
            load.start()
    load_cells.start()

    barrier = pltpu.get_barrier_semaphore()
    peers = 0
    for shift_y in range(n_gy):
        for shift_z in range(n_gz):
            if shift_y or shift_z:
                target = (gx, lax.rem(gy + shift_y, n_gy), lax.rem(gz + shift_z, n_gz))
                pl.semaphore_signal(barrier, inc=1, device_id=target, device_id_type=MESH)
                peers += 1
    if n_gx > 1:
        for shift in (1, n_gx - 1):
            target = (lax.rem(gx + shift, n_gx), gy, gz)
            pl.semaphore_signal(barrier, inc=1, device_id=target, device_id_type=MESH)
            peers += 1

    load_small[2].wait()
    load_prior.wait()
    for writer in range(writers):
        outgoing[writer] = prior[:, stripe_ref[writer]]
    if peers:
        pl.semaphore_wait(barrier, peers)

    def piece(target_gy, target_gz):
        target = target_gy * n_gz + target_gz
        return pltpu.make_async_remote_copy(
            src_ref=outgoing.at[target],
            dst_ref=arrived.at[me],
            send_sem=send_sem.at[target],
            recv_sem=recv_sem.at[me],
            device_id=(gx, target_gy, target_gz),
            device_id_type=MESH,
        )

    batches = [(distance, shift_y) for distance in range(1, n_gz) for shift_y in range(n_gy)]

    def start_batch(batch):
        distance, shift_y = batch
        target_gy = lax.rem(gy + shift_y, n_gy)

        @pl.when(gz + distance < n_gz)
        def _():
            piece(target_gy, gz + distance).start()

        @pl.when(gz >= distance)
        def _():
            piece(target_gy, gz - distance).start()

    head = FIRST_BATCHES
    per_step = [batches[:head]] + [batches[head + i : head + i + 1] for i in range(STEPS - 1)]
    per_step.append(batches[head + STEPS - 1 :])
    for batch in per_step[0]:
        start_batch(batch)
    for shift_y in range(1, n_gy):
        piece(lax.rem(gy + shift_y, n_gy), gz).start()
    own = pltpu.make_async_copy(outgoing.at[me], arrived.at[me], load_sem.at[2])
    own.start()

    at_lo = {LO_T: gz == 0, LO_W: gy == 0, LO_D: gx == 0}
    at_hi = {HI_T: gz == n_gz - 1, HI_W: gy == n_gy - 1, HI_D: gx == n_gx - 1}
    landing = {
        LO_T: face_lo_t, HI_T: face_hi_t, LO_W: face_lo_w,
        HI_W: face_hi_w, LO_D: face_lo_d, HI_D: face_hi_d,
    }
    missing = {**at_lo, **at_hi}
    no_target = {
        LO_T: at_hi[HI_T], HI_T: at_lo[LO_T], LO_W: at_hi[HI_W],
        HI_W: at_lo[LO_W], LO_D: at_hi[HI_D], HI_D: at_lo[LO_D],
    }
    for face, ref in landing.items():
        @pl.when(missing[face])
        def _(ref=ref):
            ref[...] = jnp.zeros_like(ref)

    def face_copy(step, face):
        sources = {
            LO_T: (excited.at[step, cells_t - 1], (gx, gy, gz + 1)),
            HI_T: (excited.at[step, 0], (gx, gy, gz - 1)),
            LO_W: (excited.at[step, :, pl.ds(cells_w - SUB, SUB), :], (gx, gy + 1, gz)),
            HI_W: (excited.at[step, :, pl.ds(0, SUB), :], (gx, gy - 1, gz)),
            LO_D: (excited.at[step, :, :, pl.ds(cells_d - LANES, LANES)], (gx + 1, gy, gz)),
            HI_D: (excited.at[step, :, :, pl.ds(0, LANES)], (gx - 1, gy, gz)),
        }
        source, target = sources[face]
        return pltpu.make_async_remote_copy(
            src_ref=source,
            dst_ref=landing[face].at[step],
            send_sem=face_send.at[step, face],
            recv_sem=face_recv.at[step, face],
            device_id=target,
            device_id_type=MESH,
        )

    for i, load in enumerate(load_small):
        if i != 2:
            load.wait()
    classes = fibers_ref[...]
    picked = [jnp.full(classes.shape, conduct_ref[c, 0], jnp.float32) for c in range(3)]
    for fiber in range(1, conduct_ref.shape[1]):
        hit = classes == fiber
        picked = [jnp.where(hit, conduct_ref[c, fiber], old) for c, old in enumerate(picked)]
    for c in range(3):
        sigma[c] = picked[c]

    load_cells.wait()
    slab = max(1, cells_t // 2)

    def ionic(step):
        for first in range(0, cells_t, slab):
            span = pl.ds(first, slab)
            voltage = cells[0, span]
            layer = layers_ref[span]
            hits = [layer == which for which in range(layer_count - 1)]

            def pick(table, gate):
                value = jnp.full(voltage.shape, table[layer_count - 1, gate], jnp.float32)
                for which in range(layer_count - 2, -1, -1):
                    value = jnp.where(hits[which], table[which, gate], value)
                return value

            def one_gate(gate, current):
                steady = 1.0 / (
                    1.0 + jnp.exp((pick(half_ref, gate) - voltage) * pick(slope_ref, gate))
                )
                decay = jnp.exp(-1.0 / (pick(tau_ref, gate) * (1.0 + steady)))
                value = steady + (cells[gate + 1, span] - steady) * decay
                cells[gate + 1, span] = value
                return current + pick(cond_ref, gate) * value * (voltage - pick(rev_ref, gate))

            current = lax.fori_loop(0, gates, one_gate, jnp.zeros_like(voltage))
            excited[step, span] = voltage - current

    flat = (cells_t * cells_w, cells_d)
    row = lax.broadcasted_iota(jnp.int32, flat, 0) % cells_w
    lane = lax.broadcasted_iota(jnp.int32, flat, 1)

    def factor(flag):
        return 1.0 - flag.astype(jnp.float32)

    def spread(rows_value):
        return jnp.broadcast_to(rows_value, (cells_t, cells_w, cells_d)).reshape(flat)

    def diffuse(step):
        centre3 = excited[step]
        centre = centre3.reshape(flat)
        below = jnp.concatenate([face_lo_t[step][None], centre3[:-1]], axis=0) - centre3
        above = jnp.concatenate([centre3[1:], face_hi_t[step][None]], axis=0) - centre3
        slab_index = lax.broadcasted_iota(jnp.int32, centre3.shape, 0)
        below = jnp.where(slab_index == 0, below * factor(missing[LO_T]), below)
        above = jnp.where(slab_index == cells_t - 1, above * factor(missing[HI_T]), above)
        across = (below + above).reshape(flat)

        low = spread(face_lo_w[step][:, SUB - 1 : SUB, :])
        high = spread(face_hi_w[step][:, 0:1, :])
        below = jnp.where(
            row == 0, (low - centre) * factor(missing[LO_W]), pltpu.roll(centre, 1, 0) - centre
        )
        above = jnp.where(
            row == cells_w - 1,
            (high - centre) * factor(missing[HI_W]),
            pltpu.roll(centre, flat[0] - 1, 0) - centre,
        )
        widthwise = below + above

        low = pltpu.roll(face_lo_d[step].reshape(flat[0], LANES), 1, 1)
        high = pltpu.roll(face_hi_d[step].reshape(flat[0], LANES), LANES - 1, 1)
        low = jnp.concatenate([low] * (cells_d // LANES), axis=1)
        high = jnp.concatenate([high] * (cells_d // LANES), axis=1)
        below = jnp.where(
            lane == 0, (low - centre) * factor(missing[LO_D]), pltpu.roll(centre, 1, 1) - centre
        )
        above = jnp.where(
            lane == cells_d - 1,
            (high - centre) * factor(missing[HI_D]),
            pltpu.roll(centre, cells_d - 1, 1) - centre,
        )
        depthwise = below + above
        voltage = (
            centre
            + sigma[0].reshape(flat) * across
            + sigma[1].reshape(flat) * widthwise
            + sigma[2].reshape(flat) * depthwise
        )
        cells[0] = voltage.reshape(centre3.shape)

    for step in range(STEPS):
        ionic(step)
        for face in range(6):
            @pl.when(jnp.logical_not(no_target[face]))
            def _(face=face):
                face_copy(step, face).start()
        for batch in per_step[step + 1]:
            start_batch(batch)
        for face in range(6):
            @pl.when(jnp.logical_not(missing[face]))
            def _(face=face):
                face_copy(step, face).wait_recv()
        diffuse(step)

    for step in range(STEPS):
        for face in range(6):
            @pl.when(jnp.logical_not(no_target[face]))
            def _(face=face, step=step):
                face_copy(step, face).wait_send()
    own.wait()
    for shift_y in range(n_gy):
        for shift_z in range(n_gz):
            if shift_y or shift_z:
                source_gy = lax.rem(gy + shift_y, n_gy)
                source_gz = lax.rem(gz + shift_z, n_gz)
                source = source_gy * n_gz + source_gz
                piece(source_gy, source_gz).wait_send()
                pltpu.make_async_remote_copy(
                    src_ref=outgoing.at[source],
                    dst_ref=arrived.at[source],
                    send_sem=send_sem.at[source],
                    recv_sem=recv_sem.at[source],
                    device_id=(gx, source_gy, source_gz),
                    device_id_type=MESH,
                ).wait_recv()


def write_out(cells, arrived, new_hbm, stripes_hbm, sem):
    writers, count = arrived.shape[0], cells.shape[0]
    copies = [
        pltpu.make_async_copy(arrived.at[q], stripes_hbm.at[:, q], sem.at[q])
        for q in range(writers)
    ]
    bounds = [count * cut // OUT_CUTS for cut in range(OUT_CUTS + 1)]
    for cut, (first, last) in enumerate(zip(bounds, bounds[1:])):
        span = pl.ds(first, last - first)
        copies.append(
            pltpu.make_async_copy(cells.at[span], new_hbm.at[span], sem.at[writers + cut])
        )
    for copy in copies:
        copy.start()
    for copy in copies:
        copy.wait()


def per_device(sizes, states, prior_states, cell_layers, fiber_classes, writer_stripe, *tables):
    n_gx, n_gy, n_gz = sizes
    writers = n_gy * n_gz
    count, cells_t, cells_w, cells_d = states.shape
    rows = cells_t * cells_w // writers
    f32 = jnp.float32
    tables = tables[:-1] + (tables[-1].T,)
    hbm = pl.BlockSpec(memory_space=pltpu.HBM)
    vmem = pl.BlockSpec(memory_space=pltpu.VMEM)
    new_states, arrived = pl.pallas_call(
        functools.partial(kernel, sizes),
        out_shape=(
            pltpu.VMEM(states.shape, f32),
            pltpu.VMEM((writers, count, rows, cells_d), f32),
        ),
        in_specs=[hbm] * 11,
        out_specs=(vmem, vmem),
        scratch_shapes=[
            pltpu.VMEM(cell_layers.shape, jnp.int32),
            pltpu.VMEM(cell_layers.shape, jnp.int32),
            pltpu.SMEM(writer_stripe.shape, jnp.int32),
            *[pltpu.SMEM(table.shape, f32) for table in tables],
            pltpu.VMEM((count, writers, rows, cells_d), f32),
            pltpu.VMEM((writers, count, rows, cells_d), f32),
            pltpu.VMEM((STEPS, cells_t, cells_w, cells_d), f32),
            pltpu.VMEM((STEPS, cells_w, cells_d), f32),
            pltpu.VMEM((STEPS, cells_w, cells_d), f32),
            pltpu.VMEM((STEPS, cells_t, SUB, cells_d), f32),
            pltpu.VMEM((STEPS, cells_t, SUB, cells_d), f32),
            pltpu.VMEM((STEPS, cells_t, cells_w, LANES), f32),
            pltpu.VMEM((STEPS, cells_t, cells_w, LANES), f32),
            pltpu.VMEM((3, cells_t, cells_w, cells_d), f32),
            pltpu.SemaphoreType.DMA((3,)),
            pltpu.SemaphoreType.DMA((9,)),
            pltpu.SemaphoreType.DMA((writers,)),
            pltpu.SemaphoreType.DMA((writers,)),
            pltpu.SemaphoreType.DMA((STEPS, 6)),
            pltpu.SemaphoreType.DMA((STEPS, 6)),
        ],
        compiler_params=pltpu.CompilerParams(
            collective_id=0, has_side_effects=True, vmem_limit_bytes=VMEM_BYTES - 0x20000 - 2 * states.size * states.dtype.itemsize
        ),
        name="monodomain",
    )(
        states,
        prior_states.reshape(count, writers, rows, cells_d),
        cell_layers,
        fiber_classes,
        writer_stripe,
        *tables,
    )
    stripes_shape = (count, writers, rows, cells_d)
    return pl.pallas_call(
        write_out,
        out_shape=(
            jax.ShapeDtypeStruct(states.shape, f32),
            jax.ShapeDtypeStruct(stripes_shape, f32),
        ),
        in_specs=[vmem, vmem],
        out_specs=(hbm, hbm),
        scratch_shapes=[pltpu.SemaphoreType.DMA((writers + OUT_CUTS,))],
        compiler_params=pltpu.CompilerParams(vmem_limit_bytes=1024 * 1024),
        name="write_out",
    )(new_states, arrived)


def solution(mesh):
    cells = P("gz", "gy", "gx")
    whole_states = P(None, "gz", "gy", "gx")
    sizes = (mesh.shape["gx"], mesh.shape["gy"], mesh.shape["gz"])
    return jax.shard_map(
        functools.partial(per_device, sizes),
        mesh=mesh,
        in_specs=(whole_states, whole_states, cells, cells) + (P(),) * 7,
        out_specs=(whole_states, P(None, ("gy", "gz"), None, "gx")),
        check_vma=False,
    )
```

```python
import functools

import jax
import jax.numpy as jnp
from jax import lax
from jax.experimental import pallas as pl
from jax.experimental.pallas import tpu as pltpu
from jax.sharding import PartitionSpec as P

STEPS = 4
MESH = pl.DeviceIdType.MESH
SUB = 8
LANES = 128
OUT_CUTS = 8
VMEM_BYTES = 67_043_328
FIRST_BATCHES = 1
UNROLL = 2
LOG2E = 1.4426950408889634
LO_T, HI_T, LO_W, HI_W, LO_D, HI_D = range(6)


def kernel(
    sizes,
    states_hbm,
    prior_hbm,
    *rest,
):
    small_hbm, (cells, arrived), scratch = rest[:9], rest[9:11], rest[11:]
    small, (prior, outgoing, excited, face_lo_t, face_hi_t, face_lo_w, face_hi_w, face_lo_d, face_hi_d, sigma, picked_half, picked_slope, picked_rate, picked_cond, picked_rev, load_sem, small_sem, send_sem, recv_sem, face_send, face_recv) = scratch[:9], scratch[9:]
    layers_ref, fibers_ref, stripe_ref, half_ref, slope_ref, tau_ref, cond_ref, rev_ref, conduct_ref = small
    n_gx, n_gy, n_gz = sizes
    writers = n_gy * n_gz
    states_count, cells_t, cells_w, cells_d = cells.shape
    rows = outgoing.shape[2]
    layer_count, gates = half_ref.shape
    gx, gy, gz = lax.axis_index("gx"), lax.axis_index("gy"), lax.axis_index("gz")
    me = gy * n_gz + gz

    load_prior = pltpu.make_async_copy(prior_hbm, prior, load_sem.at[0])
    load_small = [
        pltpu.make_async_copy(source, target, small_sem.at[i])
        for i, (source, target) in enumerate(zip(small_hbm, small))
    ]
    load_cells = pltpu.make_async_copy(states_hbm, cells, load_sem.at[1])
    load_small[2].start()
    load_prior.start()
    for i, load in enumerate(load_small):
        if i != 2:
            load.start()
    load_cells.start()

    barrier = pltpu.get_barrier_semaphore()
    peers = 0
    for shift_y in range(n_gy):
        for shift_z in range(n_gz):
            if shift_y or shift_z:
                target = (gx, lax.rem(gy + shift_y, n_gy), lax.rem(gz + shift_z, n_gz))
                pl.semaphore_signal(barrier, inc=1, device_id=target, device_id_type=MESH)
                peers += 1
    if n_gx > 1:
        for shift in (1, n_gx - 1):
            target = (lax.rem(gx + shift, n_gx), gy, gz)
            pl.semaphore_signal(barrier, inc=1, device_id=target, device_id_type=MESH)
            peers += 1

    load_small[2].wait()
    load_prior.wait()
    for writer in range(writers):
        outgoing[writer] = prior[:, stripe_ref[writer]]
    if peers:
        pl.semaphore_wait(barrier, peers)

    def piece(target_gy, target_gz):
        target = target_gy * n_gz + target_gz
        return pltpu.make_async_remote_copy(
            src_ref=outgoing.at[target],
            dst_ref=arrived.at[me],
            send_sem=send_sem.at[target],
            recv_sem=recv_sem.at[me],
            device_id=(gx, target_gy, target_gz),
            device_id_type=MESH,
        )

    batches = [(distance, shift_y) for distance in range(1, n_gz) for shift_y in range(n_gy)]

    def start_batch(batch):
        distance, shift_y = batch
        target_gy = lax.rem(gy + shift_y, n_gy)

        @pl.when(gz + distance < n_gz)
        def _():
            piece(target_gy, gz + distance).start()

        @pl.when(gz >= distance)
        def _():
            piece(target_gy, gz - distance).start()

    head = FIRST_BATCHES
    per_step = [batches[:head]] + [batches[head + i : head + i + 1] for i in range(STEPS - 1)]
    per_step.append(batches[head + STEPS - 1 :])
    for batch in per_step[0]:
        start_batch(batch)
    for shift_y in range(1, n_gy):
        piece(lax.rem(gy + shift_y, n_gy), gz).start()
    own = pltpu.make_async_copy(outgoing.at[me], arrived.at[me], load_sem.at[2])
    own.start()

    at_lo = {LO_T: gz == 0, LO_W: gy == 0, LO_D: gx == 0}
    at_hi = {HI_T: gz == n_gz - 1, HI_W: gy == n_gy - 1, HI_D: gx == n_gx - 1}
    landing = {
        LO_T: face_lo_t, HI_T: face_hi_t, LO_W: face_lo_w,
        HI_W: face_hi_w, LO_D: face_lo_d, HI_D: face_hi_d,
    }
    missing = {**at_lo, **at_hi}
    no_target = {
        LO_T: at_hi[HI_T], HI_T: at_lo[LO_T], LO_W: at_hi[HI_W],
        HI_W: at_lo[LO_W], LO_D: at_hi[HI_D], HI_D: at_lo[LO_D],
    }
    for face, ref in landing.items():
        @pl.when(missing[face])
        def _(ref=ref):
            ref[...] = jnp.zeros_like(ref)

    def face_copy(step, face):
        sources = {
            LO_T: (excited.at[step, cells_t - 1], (gx, gy, gz + 1)),
            HI_T: (excited.at[step, 0], (gx, gy, gz - 1)),
            LO_W: (excited.at[step, :, pl.ds(cells_w - SUB, SUB), :], (gx, gy + 1, gz)),
            HI_W: (excited.at[step, :, pl.ds(0, SUB), :], (gx, gy - 1, gz)),
            LO_D: (excited.at[step, :, :, pl.ds(cells_d - LANES, LANES)], (gx + 1, gy, gz)),
            HI_D: (excited.at[step, :, :, pl.ds(0, LANES)], (gx - 1, gy, gz)),
        }
        source, target = sources[face]
        return pltpu.make_async_remote_copy(
            src_ref=source,
            dst_ref=landing[face].at[step],
            send_sem=face_send.at[step, face],
            recv_sem=face_recv.at[step, face],
            device_id=target,
            device_id_type=MESH,
        )

    for i, load in enumerate(load_small):
        if i != 2:
            load.wait()
    classes = fibers_ref[...]
    picked = [jnp.full(classes.shape, conduct_ref[c, 0], jnp.float32) for c in range(3)]
    for fiber in range(1, conduct_ref.shape[1]):
        hit = classes == fiber
        picked = [jnp.where(hit, conduct_ref[c, fiber], old) for c, old in enumerate(picked)]
    for c in range(3):
        sigma[c] = picked[c]

    load_cells.wait()
    slab = max(1, cells_t // 2)

    def pick_tables(slab_index):
        layer = layers_ref[slab_index]
        hits = [layer == which for which in range(layer_count - 1)]

        def pick(values):
            value = jnp.full(layer.shape, values[-1], jnp.float32)
            for hit, one in reversed(list(zip(hits, values))):
                value = jnp.where(hit, one, value)
            return value

        def one_gate(gate, carry):
            def of(table):
                return [table[which, gate] for which in range(layer_count)]

            picked_half[gate, slab_index] = pick(of(half_ref))
            picked_slope[gate, slab_index] = pick(of(slope_ref)) * LOG2E
            picked_rate[gate, slab_index] = -LOG2E / pick(of(tau_ref))
            picked_cond[gate, slab_index] = pick(of(cond_ref))
            picked_rev[gate, slab_index] = pick(of(rev_ref))
            return carry

        lax.fori_loop(0, gates, one_gate, 0)

    for slab_index in range(cells_t):
        pick_tables(slab_index)

    def ionic(step):
        for first in range(0, cells_t, slab):
            span = pl.ds(first, slab)
            voltage = cells[0, span]

            def one_gate(gate, current):
                steady = 1.0 / (
                    1.0
                    + jnp.exp2((picked_half[gate, span] - voltage) * picked_slope[gate, span])
                )
                decay = jnp.exp2(picked_rate[gate, span] / (1.0 + steady))
                value = steady + (cells[gate + 1, span] - steady) * decay
                cells[gate + 1, span] = value
                return current + picked_cond[gate, span] * value * (
                    voltage - picked_rev[gate, span]
                )

            current = lax.fori_loop(
                0, gates, one_gate, jnp.zeros_like(voltage), unroll=UNROLL
            )
            excited[step, span] = voltage - current

    flat = (cells_t * cells_w, cells_d)
    row = lax.broadcasted_iota(jnp.int32, flat, 0) % cells_w
    lane = lax.broadcasted_iota(jnp.int32, flat, 1)

    def factor(flag):
        return 1.0 - flag.astype(jnp.float32)

    def spread(rows_value):
        return jnp.broadcast_to(rows_value, (cells_t, cells_w, cells_d)).reshape(flat)

    def diffuse(step):
        centre3 = excited[step]
        centre = centre3.reshape(flat)
        below = jnp.concatenate([face_lo_t[step][None], centre3[:-1]], axis=0) - centre3
        above = jnp.concatenate([centre3[1:], face_hi_t[step][None]], axis=0) - centre3
        slab_index = lax.broadcasted_iota(jnp.int32, centre3.shape, 0)
        below = jnp.where(slab_index == 0, below * factor(missing[LO_T]), below)
        above = jnp.where(slab_index == cells_t - 1, above * factor(missing[HI_T]), above)
        across = (below + above).reshape(flat)

        low = spread(face_lo_w[step][:, SUB - 1 : SUB, :])
        high = spread(face_hi_w[step][:, 0:1, :])
        below = jnp.where(
            row == 0, (low - centre) * factor(missing[LO_W]), pltpu.roll(centre, 1, 0) - centre
        )
        above = jnp.where(
            row == cells_w - 1,
            (high - centre) * factor(missing[HI_W]),
            pltpu.roll(centre, flat[0] - 1, 0) - centre,
        )
        widthwise = below + above

        low = pltpu.roll(face_lo_d[step].reshape(flat[0], LANES), 1, 1)
        high = pltpu.roll(face_hi_d[step].reshape(flat[0], LANES), LANES - 1, 1)
        low = jnp.concatenate([low] * (cells_d // LANES), axis=1)
        high = jnp.concatenate([high] * (cells_d // LANES), axis=1)
        below = jnp.where(
            lane == 0, (low - centre) * factor(missing[LO_D]), pltpu.roll(centre, 1, 1) - centre
        )
        above = jnp.where(
            lane == cells_d - 1,
            (high - centre) * factor(missing[HI_D]),
            pltpu.roll(centre, cells_d - 1, 1) - centre,
        )
        depthwise = below + above
        voltage = (
            centre
            + sigma[0].reshape(flat) * across
            + sigma[1].reshape(flat) * widthwise
            + sigma[2].reshape(flat) * depthwise
        )
        cells[0] = voltage.reshape(centre3.shape)

    for step in range(STEPS):
        ionic(step)
        for face in range(6):
            @pl.when(jnp.logical_not(no_target[face]))
            def _(face=face):
                face_copy(step, face).start()
        for batch in per_step[step + 1]:
            start_batch(batch)
        for face in range(6):
            @pl.when(jnp.logical_not(missing[face]))
            def _(face=face):
                face_copy(step, face).wait_recv()
        diffuse(step)

    for step in range(STEPS):
        for face in range(6):
            @pl.when(jnp.logical_not(no_target[face]))
            def _(face=face, step=step):
                face_copy(step, face).wait_send()
    own.wait()
    for shift_y in range(n_gy):
        for shift_z in range(n_gz):
            if shift_y or shift_z:
                source_gy = lax.rem(gy + shift_y, n_gy)
                source_gz = lax.rem(gz + shift_z, n_gz)
                source = source_gy * n_gz + source_gz
                piece(source_gy, source_gz).wait_send()
                pltpu.make_async_remote_copy(
                    src_ref=outgoing.at[source],
                    dst_ref=arrived.at[source],
                    send_sem=send_sem.at[source],
                    recv_sem=recv_sem.at[source],
                    device_id=(gx, source_gy, source_gz),
                    device_id_type=MESH,
                ).wait_recv()


def write_out(cells, arrived, new_hbm, stripes_hbm, sem):
    writers, count = arrived.shape[0], cells.shape[0]
    copies = [
        pltpu.make_async_copy(arrived.at[q], stripes_hbm.at[:, q], sem.at[q])
        for q in range(writers)
    ]
    bounds = [count * cut // OUT_CUTS for cut in range(OUT_CUTS + 1)]
    for cut, (first, last) in enumerate(zip(bounds, bounds[1:])):
        span = pl.ds(first, last - first)
        copies.append(
            pltpu.make_async_copy(cells.at[span], new_hbm.at[span], sem.at[writers + cut])
        )
    for copy in copies:
        copy.start()
    for copy in copies:
        copy.wait()


def per_device(sizes, states, prior_states, cell_layers, fiber_classes, writer_stripe, *tables):
    n_gx, n_gy, n_gz = sizes
    writers = n_gy * n_gz
    count, cells_t, cells_w, cells_d = states.shape
    rows = cells_t * cells_w // writers
    f32 = jnp.float32
    tables = tables[:-1] + (tables[-1].T,)
    hbm = pl.BlockSpec(memory_space=pltpu.HBM)
    vmem = pl.BlockSpec(memory_space=pltpu.VMEM)
    new_states, arrived = pl.pallas_call(
        functools.partial(kernel, sizes),
        out_shape=(
            pltpu.VMEM(states.shape, f32),
            pltpu.VMEM((writers, count, rows, cells_d), f32),
        ),
        in_specs=[hbm] * 11,
        out_specs=(vmem, vmem),
        scratch_shapes=[
            pltpu.VMEM(cell_layers.shape, jnp.int32),
            pltpu.VMEM(cell_layers.shape, jnp.int32),
            pltpu.SMEM(writer_stripe.shape, jnp.int32),
            *[pltpu.SMEM(table.shape, f32) for table in tables],
            pltpu.VMEM((count, writers, rows, cells_d), f32),
            pltpu.VMEM((writers, count, rows, cells_d), f32),
            pltpu.VMEM((STEPS, cells_t, cells_w, cells_d), f32),
            pltpu.VMEM((STEPS, cells_w, cells_d), f32),
            pltpu.VMEM((STEPS, cells_w, cells_d), f32),
            pltpu.VMEM((STEPS, cells_t, SUB, cells_d), f32),
            pltpu.VMEM((STEPS, cells_t, SUB, cells_d), f32),
            pltpu.VMEM((STEPS, cells_t, cells_w, LANES), f32),
            pltpu.VMEM((STEPS, cells_t, cells_w, LANES), f32),
            pltpu.VMEM((3, cells_t, cells_w, cells_d), f32),
            *[pltpu.VMEM((count - 1, cells_t, cells_w, cells_d), f32)] * 5,
            pltpu.SemaphoreType.DMA((3,)),
            pltpu.SemaphoreType.DMA((9,)),
            pltpu.SemaphoreType.DMA((writers,)),
            pltpu.SemaphoreType.DMA((writers,)),
            pltpu.SemaphoreType.DMA((STEPS, 6)),
            pltpu.SemaphoreType.DMA((STEPS, 6)),
        ],
        compiler_params=pltpu.CompilerParams(
            collective_id=0, has_side_effects=True, vmem_limit_bytes=VMEM_BYTES - 0x20000 - 2 * states.size * states.dtype.itemsize
        ),
        name="monodomain",
    )(
        states,
        prior_states.reshape(count, writers, rows, cells_d),
        cell_layers,
        fiber_classes,
        writer_stripe,
        *tables,
    )
    stripes_shape = (count, writers, rows, cells_d)
    return pl.pallas_call(
        write_out,
        out_shape=(
            jax.ShapeDtypeStruct(states.shape, f32),
            jax.ShapeDtypeStruct(stripes_shape, f32),
        ),
        in_specs=[vmem, vmem],
        out_specs=(hbm, hbm),
        scratch_shapes=[pltpu.SemaphoreType.DMA((writers + OUT_CUTS,))],
        compiler_params=pltpu.CompilerParams(vmem_limit_bytes=1024 * 1024),
        name="write_out",
    )(new_states, arrived)


def solution(mesh):
    cells = P("gz", "gy", "gx")
    whole_states = P(None, "gz", "gy", "gx")
    sizes = (mesh.shape["gx"], mesh.shape["gy"], mesh.shape["gz"])
    return jax.shard_map(
        functools.partial(per_device, sizes),
        mesh=mesh,
        in_specs=(whole_states, whole_states, cells, cells) + (P(),) * 7,
        out_specs=(whole_states, P(None, ("gy", "gz"), None, "gx")),
        check_vma=False,
    )
```
